32 devices in a mesh: seq: 4 (over x, core), fsdp: 8 (over z, y).
Axes of the slice: x: 2, y: 2, z: 4, core: 2. Of those that a mesh axis runs over, the one named last changes fastest.
Arguments:
- tokens: bfloat16 [8, 1024, 1536], P('fsdp', 'seq'), may hold values from -6 to 6
- seq_ids: int32 [8, 1024], P('fsdp'), may hold values from 0 to 3, never falling along the last dimension, each value on 1 to 512 neighbouring positions
- routes: int32 [8, 1024, 8], P('fsdp', 'seq'), may hold values from 0 to 31, all different within a row; in each aligned block of 256 rows (0 to 255, 256 to 511, ..., all dimensions but the last counted through in order) at most 80 rows name the same one
- gain_attn: bfloat16 [1536], P('fsdp'), may hold values from 0.5 to 1.5
- w_query: bfloat16 [1536, 1536], P('fsdp'), may hold values from -0.15625 to 0.15625
- key_matrix: bfloat16 [1536, 512], P('fsdp'), may hold values from -0.15625 to 0.15625
- value_matrix: bfloat16 [1536, 512], P('fsdp'), may hold values from -0.15625 to 0.15625
- w_out: bfloat16 [1536, 1536], P('fsdp'), may hold values from -1.25 to 1.25
- gain_moe: bfloat16 [1536], P('fsdp'), may hold values from 0.5 to 1.5
- w_router: bfloat16 [1536, 32], P('fsdp'), may hold values from -0.3125 to 0.3125
- w_gate: bfloat16 [32, 1536, 512], P('fsdp'), may hold values from -0.15625 to 0.15625
- w_up: bfloat16 [32, 1536, 512], P('fsdp'), may hold values from -0.15625 to 0.15625
- w_down: bfloat16 [32, 512, 1536], P('fsdp'), may hold values from -1 to 1
- grad_out: bfloat16 [8, 1024, 1536], P('fsdp', 'seq'), may hold values from -6 to 6
Outputs:
- layer_out: bfloat16 [8, 1024, 1536], P('fsdp', 'seq')
- grad_tokens: bfloat16 [8, 1024, 1536], P('fsdp', 'seq')
- grad_gain_attn: float32 [1536], P('fsdp')
- grad_w_query: float32 [1536, 1536], P('fsdp')
- grad_w_key: float32 [1536, 512], P('fsdp')
- grad_w_value: float32 [1536, 512], P('fsdp')
- grad_w_out: float32 [1536, 1536], P('fsdp')
- grad_gain_moe: float32 [1536], P('fsdp')
- grad_w_router: float32 [1536, 32], P('fsdp')
- grad_w_gate: float32 [32, 1536, 512], P('fsdp')
- grad_w_up: float32 [32, 1536, 512], P('fsdp')
- grad_w_down: float32 [32, 512, 1536], P('fsdp')
The draws below stay inside these ranges and needn't reach their ends.
Inputs may be any that keep to these rules, and one draw needn't show every extreme that they name: `seq_ids`: document numbers never fall along a sequence; each document has 1 to 512 positions, and one has exactly 512. `routes`: each token names 8 different experts. Within each aligned block of 256 positions of a sequence, no expert is named by more than 80 tokens, and in some block one is named by exactly 80.
All inputs are finite; a program needn't handle non-finite values.
Results may differ from the reference program's by a relative error of at most 0.025.
Values may be sent and summed in bfloat16 or wider, within the bound.
A program may use at most 256 MiB of HBM per device.

```python
import math
import jax
import jax.numpy as jnp
import numpy as np
from jax import lax

MODEL_DIMENSION = 1536
QUERY_HEADS = 24
KEY_VALUE_HEADS = 8
HEAD_DIMENSION = 64
FF = 512
TOPK = 8
EXPERTS = 32
DOCS = 4
TOK_DEV = 256
SEQS = 8
LEN = 1024
CAP = 80


def block_levels(own_key, shape, cuts, low, largest):
    def one(position, parts):
        heights = jax.random.uniform(jax.random.fold_in(jax.random.fold_in(own_key, 6), position), (parts,), jnp.float32, low / len(cuts), largest / len(cuts))
        return jnp.repeat(jnp.exp(heights), shape[position] // parts).reshape((-1,) + (1,) * (len(shape) - position - 1))

    factor_of = one(*cuts[0])
    for cut in cuts[1:]:
        factor_of = factor_of * one(*cut)
    return factor_of


def length_profile(number_of, total, reach, lean):
    weights = [(1 << 20) // math.isqrt(grade ** lean) + 1 for grade in range(2, number_of + 1)]
    surplus, holding = total - reach - (number_of - 1), [1] * (number_of - 1)
    while surplus > 0:
        candidates = [i for i in range(number_of - 1) if holding[i] < reach]
        whole, budget = sum([weights[i] for i in candidates]), surplus
        for i in candidates:
            extra = min(reach - holding[i], max(1, budget * weights[i] // whole), surplus)
            holding[i] = holding[i] + extra
            surplus = surplus - extra
    return np.array([reach] + holding)


def uneven_parts(own_key, amount, total, most, skew):
    if amount == 2:
        one = jax.random.randint(own_key, (), max(1, total - most), min(most, total - 1) + 1)
        return jnp.stack([one, total - one])
    lengths = jnp.asarray(length_profile(amount, total, most, skew), jnp.int32)
    couples = (amount - 1) // 2
    giver, taker = lengths[1:1 + 2 * couples:2], lengths[2:2 + 2 * couples:2]
    margin = jnp.minimum(giver - 1, most - taker)
    moved = jax.random.randint(jax.random.fold_in(own_key, 1), (couples,), 0, 1 << 20) % (margin + 1)
    lengths = lengths.at[1:1 + 2 * couples:2].set(giver - moved).at[2:2 + 2 * couples:2].set(taker + moved)
    return lengths[jax.random.permutation(jax.random.fold_in(own_key, 2), amount)]


def deal_out(own_key, own, number, rows, number_of, top, reach, slope):
    ranking = jax.random.permutation(own_key, number_of)
    packed, common = shares(number_of, rows * top, reach, slope, True), shares(number_of, rows * top, reach, slope, False)
    places = jnp.arange(number_of)

    def named(tallies, offset_by):
        used = int((tallies > 0).sum())
        fixed = max(1, used // 4)
        moved = fixed + (places - fixed + offset_by * (used - fixed)) % max(1, number_of - fixed)
        return jnp.zeros((number_of,), jnp.int32).at[ranking[jnp.where(places < fixed, places, moved)]].set(jnp.asarray(tallies, jnp.int32))

    tallies = jnp.where(number % 4 == 0, named(packed, number // 4), named(common, number - number // 4 - 1))
    mixed = jax.random.permutation(jax.random.fold_in(own, 3), number_of)
    donor, receiver = mixed[0:number_of // 2 * 2:2], mixed[1:number_of // 2 * 2:2]
    slack = jnp.minimum(tallies[donor] - 1, reach - tallies[receiver]) // 2
    slack = jnp.where((donor == ranking[0]) | (receiver == ranking[0]) | (tallies[receiver] == 0), 0, jnp.maximum(slack, 0))
    moved = jax.random.randint(jax.random.fold_in(own, 4), (number_of // 2,), 0, 1 << 20) % (slack + 1)
    tallies = tallies.at[donor].add(-moved).at[receiver].add(moved)
    members = jnp.searchsorted(jnp.cumsum(tallies), jnp.arange(rows * top), side="right").astype(jnp.int32)
    listing = members.reshape(top, rows).T
    listing = listing[jax.random.permutation(jax.random.fold_in(own, 1), rows)]
    offset_by = jax.random.randint(jax.random.fold_in(own, 2), (rows, 1), 0, top)
    return jnp.take_along_axis(listing, (jnp.arange(top)[None, :] + offset_by) % top, axis=1)


def shares(count, total, reach, slope, full):
    weights = [(1 << 20) // math.isqrt(rank ** slope) + 1 for rank in range(1, count + 1)]
    largest = reach if full else min(reach, max(-(-total // count), total * weights[0] // sum(weights)))
    least = 1 if total - largest >= count - 1 else 0
    counts, spare = [largest] + [least] * (count - 1), total - largest - least * (count - 1)
    while spare > 0:
        free = [i for i in range(1, count) if counts[i] < largest] or [i for i in range(1, count) if counts[i] < reach]
        whole, budget = sum([weights[i] for i in free]), spare
        for i in free:
            addition = min(reach - counts[i], max(1, budget * weights[i] // whole), spare)
            counts[i] = counts[i] + addition
            spare = spare - addition
    return np.array(counts)


def noise(rng, shape, width, reach, pieces=(), held_as=jnp.bfloat16):
    result = jax.random.normal(rng, shape, jnp.float32) * width
    if len(pieces) > 0:
        result = block_levels(rng, shape, pieces, -0.22, 0.18) * result
    return jnp.clip(result, min=-reach, max=reach).astype(held_as)


def setup_inputs(seed: int = 0) -> dict:
    key_of = jax.random.split(jax.random.key(seed), 15)
    tokens = noise(key_of[0], (SEQS, LEN, MODEL_DIMENSION), 1.0, 6.0, ((0, 8), (1, 4)))
    seq_ids = jax.vmap(lambda own: jnp.searchsorted(jnp.cumsum(uneven_parts(own, DOCS, LEN, LEN // 2, 0)), jnp.arange(LEN), side="right"))(jax.random.split(key_of[1], SEQS)).reshape((SEQS, LEN)).astype(jnp.int32)
    routes_keys = jax.random.split(jax.random.fold_in(key_of[2], 1), SEQS * LEN // TOK_DEV)
    routes_turns = jax.random.permutation(jax.random.fold_in(key_of[2], 3), SEQS * LEN // TOK_DEV)
    routes = jax.vmap(lambda own, number: deal_out(jax.random.fold_in(key_of[2], 2), own, number, TOK_DEV, EXPERTS, TOPK, CAP, 0))(routes_keys, routes_turns).reshape((SEQS, LEN, TOPK))
    gain_attn = jnp.clip(1.0 + 0.1 * jax.random.normal(key_of[3], (MODEL_DIMENSION,), jnp.float32), 0.5, 1.5).astype(jnp.bfloat16)
    w_query = noise(key_of[4], (MODEL_DIMENSION, QUERY_HEADS * HEAD_DIMENSION), MODEL_DIMENSION ** -0.5, 0.15625, ((0, 8),))
    key_matrix = noise(key_of[5], (MODEL_DIMENSION, KEY_VALUE_HEADS * HEAD_DIMENSION), MODEL_DIMENSION ** -0.5, 0.15625, ((0, 8),))
    value_matrix = noise(key_of[6], (MODEL_DIMENSION, KEY_VALUE_HEADS * HEAD_DIMENSION), MODEL_DIMENSION ** -0.5, 0.15625, ((0, 8),))
    w_out = noise(key_of[7], (QUERY_HEADS * HEAD_DIMENSION, MODEL_DIMENSION), (QUERY_HEADS * HEAD_DIMENSION // 64) ** -0.5, 1.25, ((0, 8),))
    gain_moe = jnp.clip(1.0 + 0.1 * jax.random.normal(key_of[8], (MODEL_DIMENSION,), jnp.float32), 0.5, 1.5).astype(jnp.bfloat16)
    w_router = noise(key_of[9], (MODEL_DIMENSION, EXPERTS), (MODEL_DIMENSION // 4) ** -0.5, 0.3125, ((0, 8),))
    w_gate = noise(key_of[10], (EXPERTS, MODEL_DIMENSION, FF), MODEL_DIMENSION ** -0.5, 0.15625, ((0, 8),))
    w_up = noise(key_of[11], (EXPERTS, MODEL_DIMENSION, FF), MODEL_DIMENSION ** -0.5, 0.15625, ((0, 8),))
    w_down = noise(key_of[12], (EXPERTS, FF, MODEL_DIMENSION), (FF // 16) ** -0.5, 1.0, ((0, 8),))
    grad_out = noise(key_of[13], (SEQS, LEN, MODEL_DIMENSION), 1.0, 6.0, ((0, 8), (1, 4)))
    return {"tokens": tokens, "seq_ids": seq_ids, "routes": routes, "gain_attn": gain_attn, "w_query": w_query, "key_matrix": key_matrix, "value_matrix": value_matrix, "w_out": w_out, "gain_moe": gain_moe, "w_router": w_router, "w_gate": w_gate, "w_up": w_up, "w_down": w_down, "grad_out": grad_out}


@jax.custom_vjp
def reduced_precision(v):
    return lax.optimization_barrier(v.astype(jnp.bfloat16)).astype(jnp.float32)

@jax.custom_vjp
def reduced_precision_return(v):
    return v

def low_keep(v):
    return (reduced_precision(v), None)

def low_pass(kept, grad):
    return (grad,)

def back_keep(v):
    return (v, None)

def back_low(kept, grad):
    return (reduced_precision(grad),)
reduced_precision.defvjp(low_keep, low_pass)
reduced_precision_return.defvjp(back_keep, back_low)
norm_eps = 1e-06
highest = lax.Precision.HIGHEST

def rms_scale(values, gain):
    return values * lax.rsqrt(lax.optimization_barrier(jnp.mean(values * values, axis=-1, keepdims=True)) + norm_eps) * gain

def rotary_embedding(values, token_places, turn_sign):
    half_dim = values.shape[-1] // 2
    inv_freq = 10000.0 ** (-2.0 * jnp.arange(half_dim).astype(jnp.float32) / values.shape[-1])
    phase_angle = turn_sign * token_places.astype(jnp.float32)[:, None] * inv_freq[None, :]
    cosine = jnp.cos(phase_angle)[:, None, :]
    sine = jnp.sin(phase_angle)[:, None, :]
    first_half = values[..., :half_dim]
    second_half = values[..., half_dim:]
    return jnp.concatenate([first_half * cosine - second_half * sine, second_half * cosine + first_half * sine], axis=-1)

def layer_one(seq_rows, doc_ids, expert_ids, weights):
    gain_attn, w_query, key_matrix, value_matrix, w_out, gain_moe, w_router, w_gate, w_up, w_down = weights
    document_length = seq_rows.shape[0]
    query_group_width = QUERY_HEADS // KEY_VALUE_HEADS
    token_places = jnp.arange(document_length)
    h_attn = reduced_precision(rms_scale(seq_rows, gain_attn))
    q_lin = reduced_precision_return(jnp.dot(h_attn, w_query, precision=highest))
    key_linear = reduced_precision_return(jnp.dot(h_attn, key_matrix, precision=highest))
    value_linear = jnp.dot(h_attn, value_matrix, precision=highest)
    query_rows_projected = reduced_precision_return(reduced_precision(rotary_embedding(q_lin.reshape(document_length, QUERY_HEADS, HEAD_DIMENSION), token_places, 1.0)))
    projected_key_rows = reduced_precision_return(reduced_precision(rotary_embedding(key_linear.reshape(document_length, KEY_VALUE_HEADS, HEAD_DIMENSION), token_places, 1.0)))
    projected_value_rows = reduced_precision_return(reduced_precision(value_linear.reshape(document_length, KEY_VALUE_HEADS, HEAD_DIMENSION)))
    query_rows_projected = query_rows_projected.reshape(document_length, KEY_VALUE_HEADS, query_group_width, HEAD_DIMENSION)
    scores = reduced_precision_return(jnp.einsum('qhgd,khd->hgqk', query_rows_projected, projected_key_rows, precision=highest) * HEAD_DIMENSION ** (-0.5))
    allowed = (token_places[None, :] <= token_places[:, None]) & (doc_ids[None, :] == doc_ids[:, None])
    scores = jnp.where(allowed, scores, -1e+30)
    attn_prob = jax.nn.softmax(scores, axis=-1)
    attended = jnp.einsum('hgqk,khd->qhgd', reduced_precision(attn_prob), projected_value_rows, precision=highest)
    attended = reduced_precision_return(reduced_precision(attended.reshape(document_length, QUERY_HEADS * HEAD_DIMENSION)))
    after_attn = seq_rows + reduced_precision_return(jnp.dot(attended, w_out, precision=highest))
    h_moe = reduced_precision(rms_scale(after_attn, gain_moe))
    logits = reduced_precision_return(jnp.dot(h_moe, w_router, precision=highest))
    chosen = jnp.take_along_axis(logits, expert_ids, axis=1)
    gate_mix = jax.nn.softmax(chosen, axis=-1)
    block_count = document_length // TOK_DEV
    flat_ids = expert_ids.reshape(block_count, TOK_DEV * TOPK)
    onehot = (flat_ids[..., None] == jnp.arange(EXPERTS)).astype(jnp.int32)
    slot_rank = lax.optimization_barrier(jnp.sum((jnp.cumsum(onehot, axis=1) - 1) * onehot, axis=-1))
    slot_index = flat_ids * CAP + slot_rank
    block_index = jnp.arange(block_count)[:, None]
    token_rows = h_moe.reshape(block_count, TOK_DEV, MODEL_DIMENSION)
    taken_rows = token_rows[:, jnp.arange(TOK_DEV * TOPK) // TOPK]
    slot_rows = jnp.zeros((block_count, EXPERTS * CAP, MODEL_DIMENSION), jnp.float32).at[block_index, slot_index].set(taken_rows)
    slot_rows = reduced_precision_return(slot_rows).reshape(block_count, EXPERTS, CAP, MODEL_DIMENSION)
    gate_pre = reduced_precision_return(jnp.einsum('becd,edf->becf', slot_rows, w_gate, precision=highest))
    up_pre = reduced_precision_return(jnp.einsum('becd,edf->becf', slot_rows, w_up, precision=highest))
    hidden = reduced_precision_return(reduced_precision(jax.nn.silu(gate_pre) * up_pre))
    expert_rows = reduced_precision_return(reduced_precision(jnp.einsum('becf,efd->becd', hidden, w_down, precision=highest)))
    returned = expert_rows.reshape(block_count, EXPERTS * CAP, MODEL_DIMENSION)[block_index, slot_index]
    returned = returned.reshape(document_length, TOPK, MODEL_DIMENSION)
    return after_attn + lax.optimization_barrier(jnp.sum(gate_mix[..., None] * returned, axis=1))

def reference(tokens, seq_ids, routes, gain_attn, w_query, key_matrix, value_matrix, w_out, gain_moe, w_router, w_gate, w_up, w_down, grad_out):
    float_args = tuple((array_in.astype(jnp.float32) for array_in in (tokens, gain_attn, w_query, key_matrix, value_matrix, w_out, gain_moe, w_router, w_gate, w_up, w_down)))

    def forward(token_rows, *weights):

        def scan_step(carry_value, seq_item):
            seq_rows, doc_ids, expert_ids = seq_item
            return (carry_value, jax.checkpoint(layer_one)(seq_rows, doc_ids, expert_ids, weights))
        unused, stacked = lax.scan(scan_step, jnp.zeros((), jnp.float32), (token_rows, seq_ids, routes))
        return stacked
    layer_out, pull_back = jax.vjp(forward, *float_args)
    grad_list = pull_back(grad_out.astype(jnp.float32))
    return (layer_out.astype(jnp.bfloat16), grad_list[0].astype(jnp.bfloat16), grad_list[1], grad_list[2], grad_list[3], grad_list[4], grad_list[5], grad_list[6], grad_list[7], grad_list[8], grad_list[9], grad_list[10])
```

```python
import functools

import jax
import jax.numpy as jnp
from jax import lax
from jax.experimental import pallas as pl
from jax.experimental.pallas import tpu as pltpu
from jax.sharding import PartitionSpec as P

QUERY_HEADS = 24
KEY_VALUE_HEADS = 8
HEAD = 64
TOPK = 8
EXPERTS = 32
CAP = 80
DOC_MAX = 512
EPS = 1e-06
NEG = -1e30
F32 = jnp.float32
BF16 = jnp.bfloat16


ANY = pl.BlockSpec(memory_space=pl.ANY)
VM = pl.BlockSpec(memory_space=pltpu.VMEM)
SM = pl.BlockSpec(memory_space=pltpu.SMEM)


def sds(shape, dtype):
    return jax.ShapeDtypeStruct(shape, dtype)


def dot(a, b):
    return lax.dot_general(a, b, (((1,), (0,)), ((), ())), preferred_element_type=F32)


def dot_nt(a, b):
    return lax.dot_general(a, b, (((1,), (1,)), ((), ())), preferred_element_type=F32)


def dot_tn(a, b):
    return lax.dot_general(a, b, (((0,), (0,)), ((), ())), preferred_element_type=F32)


def cost(flops, nbytes):
    return pl.CostEstimate(flops=int(flops), bytes_accessed=int(nbytes), transcendentals=0)


SEQ_CORE = [(0, 1), (1, 0), (2, 3), (3, 2)]
SEQ_X = [(0, 2), (2, 0), (1, 3), (3, 1)]


def ring_order(n):
    return [2 * p if p < n // 2 else 2 * (n - 1 - p) + 1 for p in range(n)]


def ring_perms(n):
    order = ring_order(n)
    fwd = [(order[i], order[(i + 1) % n]) for i in range(n)]
    return fwd, [(b, a) for a, b in fwd]


def ring_slot(position, n):
    position = position % n
    return jnp.where(position < n // 2, 2 * position, 2 * (n - 1 - position) + 1)


def ring_gather(block, n, split_last):
    fwd, bwd = ring_perms(n)
    half = n // 2
    f = b = block
    out = [(0, 0, block)]
    for k in range(1, half):
        f = lax.ppermute(f, "fsdp", fwd)
        b = lax.ppermute(b, "fsdp", bwd)
        out += [(-k, 0, f), (k, 0, b)]
    if split_last:
        h = block.shape[0] // 2
        out += [
            (half, 0, lax.ppermute(f[:h], "fsdp", fwd)),
            (half, h, lax.ppermute(b[h:], "fsdp", bwd)),
        ]
    else:
        out += [(half, 0, lax.ppermute(f, "fsdp", fwd))]
    return out


def add_low(a, b):
    return (a.astype(F32) + b.astype(F32)).astype(BF16)


def ring_scatter(contrib, n, split_last):
    fwd, bwd = ring_perms(n)
    half = n // 2
    far = contrib(half)
    f = b = None
    if split_last:
        h = far.shape[0] // 2
        f = lax.ppermute(far[:h], "fsdp", fwd)
        b = lax.ppermute(far[h:], "fsdp", bwd)
    else:
        f = lax.ppermute(far, "fsdp", fwd)
    for k in range(half - 1, 0, -1):
        cf, cb = contrib(k), contrib(-k)
        if k == half - 1 and split_last:
            h = cf.shape[0] // 2
            cf = jnp.concatenate([add_low(cf[:h], f), cf[h:]], axis=0)
            cb = jnp.concatenate([cb[:h], add_low(cb[h:], b)], axis=0)
        else:
            cf = add_low(cf, f)
            cb = cb if b is None else add_low(cb, b)
        f = lax.ppermute(cf, "fsdp", fwd)
        b = lax.ppermute(cb, "fsdp", bwd)
    return contrib(0), f, b


def after(value, *others):
    return lax.optimization_barrier((value,) + tuple(others))[0]


def rms(x):
    inv = lax.rsqrt(jnp.mean(x * x, axis=-1, keepdims=True) + EPS)
    return x * inv, inv


def turn(x, cos, sin):
    lane = lax.broadcasted_iota(jnp.int32, x.shape, 1) % HEAD
    swapped = jnp.where(lane < HEAD // 2, -pltpu.roll(x, 96, 1), pltpu.roll(x, 32, 1))
    return x * cos + swapped * sin


def fetch_rows(offs, pieces, w, sems):
    copies = []
    for i, piece in enumerate(pieces):
        start = pl.multiple_of(offs[i], 16)
        copies.append(
            pltpu.make_async_copy(piece, w.at[pl.ds(start, piece.shape[0]), :], sems.at[i])
        )
    for copy in copies:
        copy.start()
    return copies


def qkv_kernel(np_, ns, cols, kvc, offs, tok, cos, sin, *refs):
    pieces = refs[:np_]
    packed, h_out, w_out, gains, w, sems, out_sem = refs[np_:]
    copies = fetch_rows(offs, pieces, w, sems)
    norm, _ = rms(tok[...].astype(F32))
    for copy in copies:
        copy.wait()
    keep = pltpu.make_async_copy(w, w_out, out_sem)
    keep.start()
    width = w.shape[1]
    extra = w[:, width - 128 :].astype(F32).T
    gains[...] = extra[32:40, :]
    h = (norm * extra[32:33, :]).astype(BF16)
    h_out[...] = h
    c, s = cos[...], sin[...]
    for j in range(ns):
        acc = dot(h, w[:, j * cols : (j + 1) * cols])
        for t in range((cols - kvc) // 128):
            part = acc[:, t * 128 : (t + 1) * 128]
            packed[j, :, t * 128 : (t + 1) * 128] = turn(part, c, s).astype(BF16)
        packed[j, :, cols - kvc :] = acc[:, cols - kvc :].astype(BF16)
    keep.wait()


def qkv_call(offs, tok, cos, sin, pieces, ns, cols, kvc):
    t, d = tok.shape
    width = pieces[0].shape[1]
    return pl.pallas_call(
        functools.partial(qkv_kernel, len(pieces), ns, cols, kvc),
        out_shape=(
            sds((ns, t, cols), BF16),
            sds((t, d), BF16),
            sds((d, width), BF16),
            sds((8, d), F32),
        ),
        in_specs=[SM, VM, VM, VM] + [ANY] * len(pieces),
        out_specs=(VM, VM, ANY, VM),
        scratch_shapes=[
            pltpu.VMEM((d, width), BF16),
            pltpu.SemaphoreType.DMA((len(pieces),)),
            pltpu.SemaphoreType.DMA,
        ],
        cost_estimate=cost(2 * t * d * width, 4 * d * width),
        name="qkv_forward",
    )(offs, tok, cos, sin, *pieces)


def head_setup(arr, q_cols, kd, vd, kt, vt, values):
    lane = lax.broadcasted_iota(jnp.int32, (arr.shape[0], 128), 1)
    k = arr[:, q_cols : q_cols + 128]
    v = arr[:, q_cols + 128 : q_cols + 256]
    kf = k.astype(F32)
    kr = pltpu.roll(kf, 64, 1)
    kd[0] = jnp.where(lane < 64, kf, kr).astype(BF16)
    kd[1] = jnp.where(lane < 64, kr, kf).astype(BF16)
    vf = v.astype(F32)
    if vd is not None:
        vr = pltpu.roll(vf, 64, 1)
        vd[0] = jnp.where(lane < 64, vf, vr).astype(BF16)
        vd[1] = jnp.where(lane < 64, vr, vf).astype(BF16)
    if kt is not None:
        kt[...] = kf.T.astype(BF16)
    if vt is not None:
        vt[...] = vf.T.astype(BF16)


def allow_mask(ids_col, ids_row, k0, k1, q0, q1):
    kpos = k0 + lax.broadcasted_iota(jnp.int32, (k1 - k0, q1 - q0), 0)
    qpos = q0 + lax.broadcasted_iota(jnp.int32, (k1 - k0, q1 - q0), 1)
    return (kpos <= qpos) & (ids_col[k0:k1, :] == ids_row[:, q0:q1])


QB = 256


def attn_fwd_kernel(heads, group, arr, ids_col, ids_row, att, lse, kd, vt, ot):
    length = arr.shape[0]
    q_cols = heads * HEAD
    head_setup(arr, q_cols, kd, None, None, vt, None)
    for q0 in range(0, length, QB):
        q1 = q0 + QB
        k0 = max(0, (q0 - DOC_MAX) // 128 * 128)
        mask = allow_mask(ids_col, ids_row, k0, q1, q0, q1)
        half_lane = lax.broadcasted_iota(jnp.int32, (QB, 128), 1) // HEAD

        def one_head(h, carry):
            g = h // group
            lanes = pl.ds(pl.multiple_of(h // 2 * 128, 128), 128)
            q = arr[q0:q1, lanes]
            q = jnp.where(half_lane == h % 2, q * 0.125, 0).astype(BF16)
            scores = jnp.where(mask, dot_nt(kd[g, k0:q1, :], q), NEG)
            peak = jnp.max(scores, axis=0, keepdims=True)
            p = jnp.exp(scores - peak)
            total = jnp.sum(p, axis=0, keepdims=True)
            lse[pl.ds(h, 1), q0:q1] = peak + jnp.log(total)
            vrows = pl.ds(pl.multiple_of(g * HEAD, HEAD), HEAD)
            o = dot(vt[vrows, k0:q1], p.astype(BF16)) / total
            ot[pl.ds(pl.multiple_of(h * HEAD, HEAD), HEAD), :] = o
            return carry

        lax.fori_loop(0, heads, one_head, 0)
        att[q0:q1, :] = ot[...].T.astype(BF16)


def attn_fwd_call(arr, ids_col, ids_row, heads, group):
    length, cols = arr.shape
    return pl.pallas_call(
        functools.partial(attn_fwd_kernel, heads, group),
        out_shape=(sds((length, heads * HEAD), BF16), sds((8, length), F32)),
        in_specs=[VM] * 3,
        out_specs=(VM, VM),
        scratch_shapes=[
            pltpu.VMEM((2, length, 128), BF16),
            pltpu.VMEM((128, length), BF16),
            pltpu.VMEM((heads * HEAD, QB), F32),
        ],
        cost_estimate=cost(16e9, 4e6),
        name="attention_forward",
    )(arr, ids_col, ids_row)


def attn_bwd_kernel(
    heads, group, arr, go, lse, ids_col, ids_row, out, kd, vd, kt, dk, dv, qt
):
    length = arr.shape[0]
    q_cols = heads * HEAD
    head_setup(arr, q_cols, kd, vd, kt, None, None)
    dk[...] = jnp.zeros_like(dk)
    dv[...] = jnp.zeros_like(dv)
    for q0 in range(0, length, QB):
        q1 = q0 + QB
        k0 = max(0, (q0 - DOC_MAX) // 128 * 128)
        mask = allow_mask(ids_col, ids_row, k0, q1, q0, q1)
        half_lane = lax.broadcasted_iota(jnp.int32, (QB, 128), 1) // HEAD

        def one_head(h, carry):
            g = h // group
            lanes = pl.ds(pl.multiple_of(h // 2 * 128, 128), 128)
            mine = half_lane == h % 2
            q = jnp.where(mine, arr[q0:q1, lanes] * 0.125, 0).astype(BF16)
            do = jnp.where(mine, go[q0:q1, lanes], 0).astype(BF16)
            scores = jnp.where(mask, dot_nt(kd[g, k0:q1, :], q), NEG)
            p = jnp.exp(scores - lse[pl.ds(h, 1), q0:q1])
            dp = dot_nt(vd[g, k0:q1, :], do)
            mean = jnp.sum(p * dp, axis=0, keepdims=True)
            ds = (p * (dp - mean)).astype(BF16)
            dv[g, k0:q1, :] += dot(p.astype(BF16), do)
            dk[g, k0:q1, :] += dot(ds, q)
            krows = pl.ds(pl.multiple_of(g * HEAD, HEAD), HEAD)
            qt[pl.ds(pl.multiple_of(h * HEAD, HEAD), HEAD), :] = dot(kt[krows, k0:q1], ds) * 0.125
            return carry

        lax.fori_loop(0, heads, one_head, 0)
        out[q0:q1, :q_cols] = qt[...].T.astype(BF16)
    lane = lax.broadcasted_iota(jnp.int32, (length, 128), 1)
    for i, acc in enumerate((dk, dv)):
        a0, a1 = acc[0], acc[1]
        a0 = a0 + pltpu.roll(a0, 64, 1)
        a1 = a1 + pltpu.roll(a1, 64, 1)
        start = q_cols + i * 128
        out[:, start : start + 128] = jnp.where(lane < 64, a0, a1).astype(BF16)


def attn_bwd_call(arr, go, lse, ids_col, ids_row, heads, group):
    length, cols = arr.shape
    return pl.pallas_call(
        functools.partial(attn_bwd_kernel, heads, group),
        out_shape=sds((length, cols), BF16),
        in_specs=[VM] * 5,
        out_specs=VM,
        scratch_shapes=[
            pltpu.VMEM((2, length, 128), BF16),
            pltpu.VMEM((2, length, 128), BF16),
            pltpu.VMEM((128, length), BF16),
            pltpu.VMEM((2, length, 128), F32),
            pltpu.VMEM((2, length, 128), F32),
            pltpu.VMEM((heads * HEAD, QB), F32),
        ],
        cost_estimate=cost(30e9, 4e6),
        name="attention_backward",
    )(arr, go, lse, ids_col, ids_row)


def out_kernel(np_, ns, offs, att, tok, gains, router, routes, *refs):
    pieces = refs[:np_]
    after_out, h_out, g_t, w_out, w, sems, out_sem = refs[np_:]
    copies = fetch_rows(offs, pieces, w, sems)
    for copy in copies:
        copy.wait()
    keep = pltpu.make_async_copy(w, w_out, out_sem)
    keep.start()
    total = tok[...].astype(F32)
    cols = att.shape[2]
    for j in range(ns):
        total = total + dot(att[j], w[j * cols : (j + 1) * cols, :])
    after_out[...] = total
    norm, _ = rms(total)
    h = (norm * gains[1:2, :]).astype(BF16)
    h_out[...] = h
    logits = dot(h, router[...])
    expert = lax.broadcasted_iota(jnp.int32, logits.shape, 1)
    named = expert == routes[:, 0:1]
    for k in range(1, TOPK):
        named = named | (expert == routes[:, k : k + 1])
    logits = jnp.where(named, logits, NEG)
    peak = jnp.max(logits, axis=1, keepdims=True)
    ex = jnp.where(named, jnp.exp(logits - peak), 0.0)
    gate = ex / jnp.sum(ex, axis=1, keepdims=True)
    g_t[...] = gate.T[:EXPERTS, :]
    keep.wait()


def out_call(offs, att, tok, gains, wext, routes, pieces):
    ns = att.shape[0]
    t, d = tok.shape
    k = ns * att.shape[2]
    n_extra = wext.shape[1] // 128 - 1
    return pl.pallas_call(
        functools.partial(out_kernel, len(pieces), ns),
        grid=(1,),
        out_shape=(sds((t, d), F32), sds((t, d), BF16), sds((EXPERTS, t), F32), sds((k, d), BF16)),
        in_specs=[SM, VM, VM, VM, pl.BlockSpec((d, 128), lambda i: (0, n_extra)), VM]
        + [ANY] * len(pieces),
        out_specs=(VM, VM, VM, ANY),
        scratch_shapes=[
            pltpu.VMEM((k, d), BF16),
            pltpu.SemaphoreType.DMA((len(pieces),)),
            pltpu.SemaphoreType.DMA,
        ],
        cost_estimate=cost(2 * t * d * k, 4 * d * k),
        name="out_projection",
    )(offs, att, tok, gains, wext, routes, *pieces)


def expert_kernel(counts, el, n_pieces, idx, *refs):
    nb = len(counts)
    pos = 0
    h_refs, z_refs = [], []
    for c in counts:
        h_refs.append(refs[pos : pos + c])
        pos += c
    for c in counts:
        z_refs.append(refs[pos : pos + c])
        pos += c
    gates, gg_in, wg, wu, wd = refs[pos : pos + 5]
    pos += 5
    y_refs = refs[pos : pos + nb]
    pos += nb
    d_refs = refs[pos : pos + nb]
    pos += nb
    x_out, z_out, hg_out, dgu_out, gg_out, xs, zs, yr, dx, pick, gslot = refs[pos:]
    e = pl.program_id(0)
    t = gates.shape[2]
    d = wg.shape[1]
    ff = wg.shape[2]
    rows_all = el * CAP

    def load(group):
        if len(group) == 1:
            return group[0][...]
        return jnp.concatenate([r[...] for r in group], axis=0)

    @pl.when(e == 0)
    def _():
        gg_out[...] = gg_in[...]
        before = (
            lax.broadcasted_iota(jnp.int32, (t, t), 0) < lax.broadcasted_iota(jnp.int32, (t, t), 1)
        ).astype(BF16)
        slot = lax.broadcasted_iota(jnp.int32, (CAP, t), 0).astype(F32)
        for b in range(nb):
            gate = gates[idx[b]]
            live = gate > 0.0
            rank = dot(live.astype(BF16), before)
            rank = jnp.where(live, rank, -1.0)
            for i in range(el):
                hit = slot == rank[i : i + 1, :]
                pick[b, i * CAP : (i + 1) * CAP, :] = hit.astype(BF16)
                gslot[b, i * CAP : (i + 1) * CAP, :] = jnp.sum(
                    jnp.where(hit, gate[i : i + 1, :], 0.0), axis=1, keepdims=True
                )
            xs[b] = dot(pick[b], load(h_refs[b])).astype(BF16)
            zs[b] = dot(pick[b], load(z_refs[b])).astype(BF16)

    rows = pl.ds(pl.multiple_of(e * CAP, 16), CAP)
    total = nb * CAP
    x = xs[:, rows, :].reshape(total, d)
    z = zs[:, rows, :].reshape(total, d)
    g = gslot[:, rows, :].reshape(total, 1)
    x_out[0] = x
    z_out[0] = z
    gate_pre = dot(x, wg[0])
    up_pre = dot(x, wu[0])
    u = dot_nt(z, wd[0])
    sig = jax.nn.sigmoid(gate_pre)
    act = gate_pre * sig
    hidden = (act * up_pre).astype(BF16)
    hidden_f = hidden.astype(F32)
    hg_out[0] = (hidden_f * g).astype(BF16)
    gg = jnp.sum(hidden_f * u, axis=1, keepdims=True)
    back = (u * g).astype(BF16).astype(F32)
    dg = (back * up_pre * sig * (1.0 + gate_pre * (1.0 - sig))).astype(BF16)
    du = (back * act).astype(BF16)
    dgu_out[0, :, :ff] = dg
    dgu_out[0, :, ff:] = du
    yr[:, rows, :] = (dot(hidden, wd[0]) * g).astype(BF16).reshape(nb, CAP, d)
    dx[:, rows, :] = (dot_nt(dg, wg[0]) + dot_nt(du, wu[0])).astype(BF16).reshape(nb, CAP, d)
    for b in range(nb):
        chosen = pick[b, rows, :].astype(F32)
        gg_out[idx[b], pl.ds(e, 1), :] = jnp.sum(
            chosen * gg[b * CAP : (b + 1) * CAP, :], axis=0, keepdims=True
        )

    @pl.when(e == el - 1)
    def _():
        for b in range(nb):
            y_refs[b][...] = dot_tn(pick[b], yr[b]).astype(BF16)
            d_refs[b][...] = dot_tn(pick[b], dx[b]).astype(BF16)


def expert_call(idx, h_blocks, z_blocks, gates, gg, wg, wu, wd):
    counts = [len(b) for b in h_blocks]
    nb = len(counts)
    n, el, t = gates.shape
    d, ff = wg.shape[1:]
    rows = nb * CAP
    flat = [p for b in h_blocks for p in b] + [p for b in z_blocks for p in b]

    def whole(a):
        zero = (0,) * a.ndim
        return pl.BlockSpec(a.shape, lambda e, i: zero, pipeline_mode=pl.Buffered(1))

    def by_e(*shape):
        zero = (0,) * len(shape)
        return pl.BlockSpec((1,) + shape, lambda e, i: (e,) + zero)

    blk = pl.BlockSpec((t, d), lambda e, i: (0, 0))
    res = pl.pallas_call(
        functools.partial(expert_kernel, counts, el, len(flat)),
        grid_spec=pltpu.PrefetchScalarGridSpec(
            num_scalar_prefetch=1,
            grid=(el,),
            in_specs=[whole(a) for a in flat]
            + [whole(gates), whole(gg), by_e(d, ff), by_e(d, ff), by_e(ff, d)],
            out_specs=[blk] * (2 * nb)
            + [
                by_e(rows, d),
                by_e(rows, d),
                by_e(rows, ff),
                by_e(rows, 2 * ff),
                pl.BlockSpec((n, el, t), lambda e, i: (0, 0, 0)),
            ],
            scratch_shapes=[pltpu.VMEM((nb, el * CAP, d), BF16)] * 4
            + [
                pltpu.VMEM((nb, el * CAP, t), BF16),
                pltpu.VMEM((nb, el * CAP, 1), F32),
            ],
        ),
        out_shape=[sds((t, d), BF16)] * (2 * nb)
        + [
            sds((el, rows, d), BF16),
            sds((el, rows, d), BF16),
            sds((el, rows, ff), BF16),
            sds((el, rows, 2 * ff), BF16),
            sds((n, el, t), F32),
        ],
        cost_estimate=cost(el * rows * d * ff * 12, el * d * ff * 6),
        name="expert_rows",
    )(idx, *flat, gates, gg, wg, wu, wd)
    return res[:nb], res[nb : 2 * nb], tuple(res[2 * nb : 2 * nb + 4]), res[-1]


def wgrad_kernel(nc, fused, hsel, *refs):
    xs, zs = refs[:nc], refs[nc : 2 * nc]
    hgs, dgus = refs[2 * nc : 3 * nc], refs[3 * nc : 4 * nc]
    pos = 4 * nc
    if fused:
        in_a, in_b = refs[pos : pos + 2]
        pos += 2
    out_a, out_b = refs[pos:]
    acc = dot_tn(xs[0][0], dgus[0][0])
    for i in range(1, nc):
        acc = acc + dot_tn(xs[i][0], dgus[i][0])
    if fused:
        acc = acc + in_a[0].astype(F32)
    out_a[0] = acc.astype(BF16)
    acc = dot_tn(hgs[0][0], zs[0][0])
    for i in range(1, nc):
        acc = acc + dot_tn(hgs[i][0], zs[i][0])
    if fused:
        acc = acc + in_b[0].astype(F32)
    out_b[0] = acc.astype(BF16)


def wgrad_call(hsel, saved, e0, ne, received=None):
    xs, zs, hgs, dgus = [list(v) for v in zip(*saved)]
    nc = len(xs)
    d = xs[0].shape[2]
    ff = hgs[0].shape[2]

    def half(a):
        return pl.BlockSpec((1, a.shape[1], a.shape[2] // 2), lambda e, s: (e + e0, 0, s[0]))

    def full(a):
        return pl.BlockSpec((1,) + a.shape[1:], lambda e, s: (e + e0, 0, 0))

    out_a = pl.BlockSpec((1, d // 2, 2 * ff), lambda e, s: (e, 0, 0))
    out_b = pl.BlockSpec((1, ff // 2, d), lambda e, s: (e, 0, 0))
    rows = sum(a.shape[1] for a in xs)
    extra = [] if received is None else list(received)
    return pl.pallas_call(
        functools.partial(wgrad_kernel, nc, received is not None),
        grid_spec=pltpu.PrefetchScalarGridSpec(
            num_scalar_prefetch=1,
            grid=(ne,),
            in_specs=[half(a) for a in xs]
            + [full(a) for a in zs]
            + [half(a) for a in hgs]
            + [full(a) for a in dgus]
            + ([out_a, out_b] if extra else []),
            out_specs=[out_a, out_b],
        ),
        out_shape=[sds((ne, d // 2, 2 * ff), BF16), sds((ne, ff // 2, d), BF16)],
        cost_estimate=cost(ne * rows * d * ff * 3, ne * rows * (d * 3 + ff * 3)),
        name="expert_weight_grads",
    )(hsel, *xs, *zs, *hgs, *dgus, *extra)


def mid_kernel(ns, d0, d1, d2, gg, g_t, after_in, gains, router, gz, wo, *refs):
    ga_out, gal_out, gatt_out, sums, grouter = refs
    gt = g_t[...]
    t = gt.shape[1]
    ggv = gg[...]
    chosen = gt * (ggv - jnp.sum(gt * ggv, axis=0, keepdims=True))
    chosen = jnp.concatenate([chosen, jnp.zeros((128 - EXPERTS, t), F32)], axis=0)
    gl = chosen.T.astype(BF16)
    gh = dot_nt(gl, router[...])
    gh = gh + (d0[...].astype(F32) + d1[...].astype(F32) + d2[...].astype(F32))
    norm, inv = rms(after_in[...])
    gain = gains[1:2, :]
    h = (norm * gain).astype(BF16)
    grouter[...] = dot_tn(h, gl)
    sums[...] = jnp.broadcast_to(jnp.sum(gh * norm, axis=0, keepdims=True), sums.shape)
    m = gh * gain
    ga = gz[...].astype(F32) + inv * (m - norm * jnp.mean(m * norm, axis=-1, keepdims=True))
    ga_out[...] = ga
    gal = ga.astype(BF16)
    gal_out[...] = gal
    cols = gatt_out.shape[2]
    for j in range(ns):
        gatt_out[j] = dot_nt(gal, wo[j * cols : (j + 1) * cols, :]).astype(BF16)


def mid_call(dh, gg, g_t, after_in, gains, wext, gz, wo, ns):
    t, d = after_in.shape
    k = wo.shape[0]
    n_extra = wext.shape[1] // 128 - 1
    return pl.pallas_call(
        functools.partial(mid_kernel, ns),
        grid=(1,),
        out_shape=(
            sds((t, d), F32),
            sds((t, d), BF16),
            sds((ns, t, k // ns), BF16),
            sds((8, d), F32),
            sds((d, 128), F32),
        ),
        in_specs=[VM] * 7 + [pl.BlockSpec((d, 128), lambda i: (0, n_extra)), VM, VM],
        out_specs=(VM,) * 5,
        cost_estimate=cost(2 * t * d * k, 2 * d * k),
        name="after_experts",
    )(*dh, gg, g_t, after_in, gains, wext, gz, wo)


def dwo_kernel(ncs, att, gal, out):
    n, r = out.shape[1], out.shape[2]
    gal_v = gal[...]
    cols = att.shape[2]
    for j in range(att.shape[0]):
        acc = dot_tn(att[j], gal_v).astype(BF16)
        for q in range(cols // r):
            block = (j * cols) // r + q
            out[block % ncs, block // ncs] = acc[q * r : (q + 1) * r, :]


def dwo_call(att, gal, n, ncs):
    ns, t, cols = att.shape
    d = gal.shape[1]
    return pl.pallas_call(
        functools.partial(dwo_kernel, ncs),
        out_shape=sds((ncs, n, ns * cols // n // ncs, d), BF16),
        in_specs=[VM, VM],
        out_specs=VM,
        cost_estimate=cost(2 * t * d * d, 2 * d * d),
        name="out_weight_grads",
    )(att, gal)


def back_kernel(ns, kvc, gp, cos, sin, w, tok, gains, ga, dq_out, gtok, sums):
    cols = gp.shape[2]
    c, s = cos[...], sin[...]
    gh = None
    for j in range(ns):
        for t in range((cols - kvc) // 128):
            part = gp[j, :, t * 128 : (t + 1) * 128].astype(F32)
            dq_out[j, :, t * 128 : (t + 1) * 128] = turn(part, c, -s).astype(BF16)
        dq_out[j, :, cols - kvc :] = gp[j, :, cols - kvc :]
        term = dot_nt(dq_out[j], w[:, j * cols : (j + 1) * cols])
        gh = term if gh is None else gh + term
    norm, inv = rms(tok[...].astype(F32))
    sums[...] = jnp.broadcast_to(jnp.sum(gh * norm, axis=0, keepdims=True), sums.shape)
    m = gh * gains[0:1, :]
    gtok[...] = (
        ga[...] + inv * (m - norm * jnp.mean(m * norm, axis=-1, keepdims=True))
    ).astype(BF16)


def back_call(gp, cos, sin, wext, tok, gains, ga, kvc):
    ns, t, cols = gp.shape
    d = tok.shape[1]
    return pl.pallas_call(
        functools.partial(back_kernel, ns, kvc),
        out_shape=(sds((ns, t, cols), BF16), sds((t, d), BF16), sds((8, d), F32)),
        in_specs=[VM] * 7,
        out_specs=(VM,) * 3,
        cost_estimate=cost(2 * t * d * cols * ns, 2 * d * cols * ns),
        name="qkv_backward",
    )(gp, cos, sin, wext, tok, gains, ga)


def dw_kernel(ncs, h, dq, extra, out):
    ns, t, cols = dq.shape
    n, r = out.shape[1], out.shape[2]
    hv = h[...]
    for j in range(ns):
        acc = dot_tn(hv, dq[j]).astype(BF16)
        for block in range(n * ncs):
            out[block % ncs, block // ncs, :, j * cols : (j + 1) * cols] = acc[
                block * r : (block + 1) * r, :
            ]
    ex = extra[...]
    for block in range(n * ncs):
        out[block % ncs, block // ncs, :, ns * cols :] = ex[block * r : (block + 1) * r, :]


def dw_call(h, dq, extra, n, ncs):
    ns, t, cols = dq.shape
    d = h.shape[1]
    width = ns * cols + 128
    return pl.pallas_call(
        functools.partial(dw_kernel, ncs),
        out_shape=sds((ncs, n, d // n // ncs, width), BF16),
        in_specs=[VM] * 3,
        out_specs=VM,
        cost_estimate=cost(2 * t * d * width, 2 * d * width),
        name="qkv_weight_grads",
    )(h, dq, extra)


def per_device(
    tokens,
    seq_ids,
    routes,
    gain_attn,
    w_query,
    key_matrix,
    value_matrix,
    w_out,
    gain_moe,
    w_router,
    w_gate,
    w_up,
    w_down,
    grad_out,
):
    ns = lax.axis_size("seq")
    n = lax.axis_size("fsdp")
    t, d = tokens.shape[1], tokens.shape[2]
    length = t * ns
    heads = QUERY_HEADS // ns
    kvh = KEY_VALUE_HEADS // ns
    group = QUERY_HEADS // KEY_VALUE_HEADS
    qc, kvc = heads * HEAD, kvh * HEAD
    cols = qc + 2 * kvc
    el = w_gate.shape[0]
    r = gain_attn.shape[0]
    half = n // 2
    seq = lax.axis_index("seq")
    f = lax.axis_index("fsdp")
    core = seq % 2
    pos = jnp.where(f % 2 == 0, f // 2, n - 1 - f // 2)
    fine = r % 64 == 0
    ncs = 2 if fine else 1

    def slot_of(rel):
        return ring_slot(pos + rel + n, n)

    def gather_rows(block):
        if not fine:
            got = ring_gather(block, n, False)
            pieces = [p for _, _, p in got]
            offs = [slot_of(rel) * r + start for rel, start, _ in got]
            return pieces, offs, got
        hr = r // 2
        mine = lax.dynamic_slice_in_dim(block, core * hr, hr, 0)
        got = ring_gather(mine, n, True)
        pieces, offs = [block], [f * r]
        for rel, start, piece in got[1:]:
            base = slot_of(rel) * r + start
            pieces += [piece, lax.ppermute(piece, "seq", SEQ_CORE)]
            offs += [base + core * hr, base + (1 - core) * hr]
        return pieces, offs, got

    tok = tokens[0]
    gz = grad_out[0]
    parts = []
    for s in range(ns):
        parts += [
            w_query[:, s * qc : (s + 1) * qc],
            key_matrix[:, s * kvc : (s + 1) * kvc],
            value_matrix[:, s * kvc : (s + 1) * kvc],
        ]
    parts += [
        w_router,
        gain_attn[:, None],
        gain_moe[:, None],
        jnp.zeros((r, 128 - EXPERTS - 2), BF16),
    ]
    pieces, offs, got = gather_rows(jnp.concatenate(parts, axis=1))
    last = [p for _, _, p in got[-2:]]
    wo_block = after(w_out, *last)
    wo_pieces, wo_offs, wo_got = gather_rows(wo_block)
    wo_last = [p for _, _, p in wo_got[-2:]]
    z_got = ring_gather(after(gz, *wo_last), n, True)

    half_dim = HEAD // 2
    inv_freq = 10000.0 ** (-2.0 * jnp.arange(half_dim).astype(F32) / HEAD)
    places = (seq * t + jnp.arange(t, dtype=jnp.int32)).astype(F32)
    angle = places[:, None] * inv_freq[None, :]
    cos = jnp.tile(jnp.cos(angle), (1, 128 // half_dim))
    sin = jnp.tile(jnp.sin(angle), (1, 128 // half_dim))
    ids_row = seq_ids
    ids_col = seq_ids.reshape(length, 1)

    packed, h_attn, wext, gains = qkv_call(
        jnp.stack(offs).astype(jnp.int32), tok, cos, sin, pieces, ns, cols, kvc
    )
    arr = lax.all_to_all(packed, "seq", split_axis=0, concat_axis=0, tiled=True)
    arr = arr.reshape(length, cols)
    att_all, lse = attn_fwd_call(arr, ids_col, ids_row, heads, group)
    att = lax.all_to_all(
        att_all.reshape(ns, t, qc), "seq", split_axis=0, concat_axis=0, tiled=True
    )
    after_attn, h_moe, g_t, wo = out_call(
        jnp.stack(wo_offs).astype(jnp.int32), att, tok, gains, wext, routes[0], wo_pieces
    )

    gates_own = g_t.reshape(n, el, t)
    gates_all = lax.all_to_all(gates_own, "fsdp", split_axis=0, concat_axis=0, tiled=True)
    h_got = ring_gather(h_moe, n, True)

    def by_rel(got_list):
        table = {}
        for rel, start, piece in got_list:
            table.setdefault(rel, []).append(piece)
        return table

    h_by, z_by = by_rel(h_got), by_rel(z_got)
    z_by[0] = [gz]
    gg = jnp.zeros((n, el, t), F32)
    y_c, d_c, saved = {}, {}, []
    chunks = [[0]] + [[-k, k] for k in range(1, half)] + [[half]]
    for chunk in chunks:
        idx = jnp.stack([slot_of(rel) for rel in chunk]).astype(jnp.int32)
        ys, ds, keep, gg = expert_call(
            idx,
            [h_by[rel] for rel in chunk],
            [z_by[rel] for rel in chunk],
            gates_own if chunk == [0] else gates_all,
            gg,
            w_gate,
            w_up,
            w_down,
        )
        for rel, y, dd in zip(chunk, ys, ds):
            y_c[rel], d_c[rel] = y, dd
        saved.append(keep)
    gg_back = lax.all_to_all(gg, "fsdp", split_axis=0, concat_axis=0, tiled=True)
    gg_back = gg_back.reshape(EXPERTS, t)
    dh = ring_scatter(lambda rel: d_c[rel], n, True)

    ne = max(1, el // 2)
    hs_send = (1 - core).reshape(1).astype(jnp.int32)
    hs_keep = core.reshape(1).astype(jnp.int32)
    chip = []
    for e0 in range(0, el, ne):
        out = wgrad_call(hs_send, saved, e0, ne)
        got_ab = [lax.ppermute(o, "seq", SEQ_CORE) for o in out]
        chip.append(wgrad_call(hs_keep, saved, e0, ne, got_ab))
    fin_own, fin_peer = [], []
    for pair in chip:
        fin = [add_low(a, lax.ppermute(a, "seq", SEQ_X)) for a in pair]
        fin_own.append(fin)
        fin_peer.append([lax.ppermute(a, "seq", SEQ_CORE) for a in fin])

    ga, gal, gatt, sums_moe, grouter = mid_call(
        dh, gg_back, g_t, after_attn, gains, wext, gz, wo, ns
    )
    go = lax.all_to_all(gatt, "seq", split_axis=0, concat_axis=0, tiled=True)
    go = go.reshape(length, qc)

    y_c = dict(zip(y_c, lax.optimization_barrier(tuple(y_c.values()) + (gatt,))[:-1]))
    y0, y1, y2 = ring_scatter(lambda rel: y_c[rel], n, True)
    layer_out = (
        after_attn + (y0.astype(F32) + y1.astype(F32) + y2.astype(F32))
    ).astype(BF16)

    def finish_rows(dw):
        if fine:
            send = lax.dynamic_index_in_dim(dw, 1 - core, 0, keepdims=False)
            keep = lax.dynamic_index_in_dim(dw, core, 0, keepdims=False)
            chip_sum = add_low(keep, lax.ppermute(send, "seq", SEQ_CORE))
        else:
            chip_sum = dw[0]
        a, b, c = ring_scatter(
            lambda rel: lax.dynamic_index_in_dim(chip_sum, slot_of(rel), 0, keepdims=False),
            n,
            fine,
        )
        total = (a.astype(F32) + b.astype(F32) + c.astype(F32)).astype(BF16)
        if not fine:
            total = add_low(total, lax.ppermute(total, "seq", SEQ_CORE))
        total = add_low(total, lax.ppermute(total, "seq", SEQ_X))
        if not fine:
            return total.astype(F32)
        other = lax.ppermute(total, "seq", SEQ_CORE)
        first = jnp.where(core == 0, total, other)
        second = jnp.where(core == 0, other, total)
        return jnp.concatenate([first, second], axis=0).astype(F32)

    grad_wout = finish_rows(dwo_call(att, gal, n, ncs))

    grad_pack = attn_bwd_call(arr, go, lse, ids_col, ids_row, heads, group)
    gp = lax.all_to_all(
        grad_pack.reshape(ns, t, cols), "seq", split_axis=0, concat_axis=0, tiled=True
    )
    dq, grad_tokens, sums_attn = back_call(gp, cos, sin, wext, tok, gains, ga, kvc)
    extra = jnp.concatenate(
        [
            grouter[:, :EXPERTS],
            sums_attn[0, :][:, None],
            sums_moe[0, :][:, None],
            jnp.zeros((d, 128 - EXPERTS - 2), F32),
        ],
        axis=1,
    ).astype(BF16)
    dwx = finish_rows(dw_call(h_attn, dq, extra, n, ncs))

    def by_seq(start, width):
        return jnp.concatenate(
            [dwx[:, s * cols + start : s * cols + start + width] for s in range(ns)], axis=1
        )

    def assemble(which):
        own = jnp.concatenate([p[which] for p in fin_own], axis=0)
        peer = jnp.concatenate([p[which] for p in fin_peer], axis=0)
        first = jnp.where(core == 0, own, peer)
        second = jnp.where(core == 0, peer, own)
        return jnp.concatenate([first, second], axis=1).astype(F32)

    ff = w_gate.shape[2]
    gu = assemble(0)
    return (
        layer_out[None],
        grad_tokens[None],
        dwx[:, ns * cols + EXPERTS],
        by_seq(0, qc),
        by_seq(qc, kvc),
        by_seq(qc + kvc, kvc),
        grad_wout,
        dwx[:, ns * cols + EXPERTS + 1],
        dwx[:, ns * cols : ns * cols + EXPERTS],
        gu[:, :, :ff],
        gu[:, :, ff:],
        assemble(1),
    )


def solution(mesh):
    row3 = P("fsdp", "seq", None)
    mat = P("fsdp", None)
    cube = P("fsdp", None, None)
    return jax.shard_map(
        per_device,
        mesh=mesh,
        in_specs=(
            row3,
            mat,
            row3,
            P("fsdp"),
            mat,
            mat,
            mat,
            mat,
            P("fsdp"),
            mat,
            cube,
            cube,
            cube,
            row3,
        ),
        out_specs=(
            row3,
            row3,
            P("fsdp"),
            mat,
            mat,
            mat,
            mat,
            P("fsdp"),
            mat,
            cube,
            cube,
            cube,
        ),
        check_vma=False,
    )
```
